32 devices in a mesh: fsdp: 8 (over y, x, core), tp: 4 (over z).
Axes of the slice: x: 2, y: 2, z: 4, core: 2. Of those that a mesh axis runs over, the one named last changes fastest.
Arguments:
- partials: bfloat16 [8, 2, 5120, 1024], P('fsdp', None, None, 'tp'), may hold values from -6 to 6
- token_counts: int32 [8], P('fsdp'), may hold values from 100 to 599
- owner_map: int32 [2, 4], replicated, may hold values from 0 to 3, each once within a row
- params: float32 [2, 5120, 1024], P(None, 'fsdp', 'tp'), may hold values from -0.75 to 0.75
- moment1: float32 [2, 5120, 1024], P(None, 'fsdp', 'tp'), may hold values from -0.15625 to 0.15625
- moment2: float32 [2, 5120, 1024], P(None, 'fsdp', 'tp'), may hold values from 0.0001 to 0.004
Outputs:
- new_params: float32 [2, 5120, 1024], P(None, 'fsdp', 'tp')
- new_moment1: float32 [2, 5120, 1024], P(None, 'fsdp', 'tp')
- new_moment2: float32 [2, 5120, 1024], P(None, 'fsdp', 'tp')
- rollout_delta: bfloat16 [2, 5120, 1024], P(None, None, 'tp')
The draws below stay inside these ranges and needn't reach their ends.
Inputs may be any that keep to these rules, and one draw needn't show every extreme that they name: `owner_map`: each row is a permutation of 0 to 3.
All inputs are finite; a program needn't handle non-finite values.
Results may differ from the reference program's by a relative error of at most 0.0004.
Values may be sent and summed in bfloat16 or wider, within the bound.
A program may use at most 64 MiB of HBM per device.

```python
import math
import jax
import jax.numpy as jnp
from jax import lax

D = 5120
KV = 1024
LAYERS = 2
STEP = 10
N_FSDP = 8
N_TP = 4


def draw_token_counts(key, part):
    base = jax.random.randint(key, (N_FSDP,), 100, 200)
    ramp = jnp.arange(N_FSDP, dtype=jnp.int32) * 400 // max(N_FSDP - 1, 1)
    position = jnp.arange(N_FSDP, dtype=jnp.int32)
    counts = jnp.where(position == 0, 100, base + ramp)
    counts = jnp.where(position == N_FSDP - 1, 599, counts)
    return counts.astype(jnp.int32)


def spiked(values, own_key, source, target, shards_of, factor):
    def block_of(dim):
        return (jnp.arange(values.shape[dim]) // (values.shape[dim] // shards_of)).reshape((-1,) + (1,) * (values.ndim - 1 - dim))

    near = jax.random.permutation(own_key, shards_of)[block_of(target)]
    far = (block_of(target) + shards_of // 2) % shards_of
    return jnp.where((block_of(source) == near) | (block_of(source) == far), factor * values, values)


def block_levels(key, shape, cuts, least, largest):
    loudness = 1.0
    for dim, blocks in cuts:
        draws = jax.random.uniform(jax.random.fold_in(jax.random.fold_in(key, 6), dim), (blocks,), jnp.float32, least / len(cuts), largest / len(cuts))
        loudness = loudness * jnp.repeat(jnp.exp(draws), shape[dim] // blocks).reshape((-1,) + (1,) * (len(shape) - 1 - dim))
    return loudness


def scatter_about(stream_key, dims, width, limit, pieces=(), held_as=jnp.bfloat16):
    drawn = jax.random.normal(stream_key, dims, jnp.float32) * width
    if len(pieces) > 0:
        drawn = block_levels(stream_key, dims, pieces, -0.22, 0.18) * drawn
    return jnp.clip(drawn, min=-limit, max=limit).astype(held_as)


def bell_draw_with(rng, extent, scale, reach, split, heavy, kind=jnp.bfloat16):
    drawn = scale * jax.random.normal(rng, extent, jnp.float32)
    if split:
        drawn = drawn * block_levels(rng, extent, split, -0.22, 0.18)
    return jnp.clip(spiked(drawn, jax.random.fold_in(rng, 3), *heavy), -reach, reach).astype(kind)


def setup_inputs(seed: int = 0) -> dict:
    streams_of = jax.random.split(jax.random.key(seed), 7)
    return {
        "partials": bell_draw_with(streams_of[0], (N_FSDP, LAYERS, D, KV), 1.0, 6.0, ((0, 8), (3, 4)), (0, 2, 8, 2.0)),
        "token_counts": draw_token_counts(jax.random.fold_in(streams_of[6], 71), 0),
        "owner_map": jax.vmap(lambda own: jax.random.permutation(own, N_TP))(jax.random.split(streams_of[2], LAYERS)).reshape((LAYERS, N_TP)).astype(jnp.int32),
        "params": scatter_about(streams_of[3], (LAYERS, D, KV), 0.05, 0.75, ((1, 8), (2, 4)), jnp.float32),
        "moment1": scatter_about(streams_of[4], (LAYERS, D, KV), 0.01, 0.15625, ((1, 8), (2, 4)), jnp.float32),
        "moment2": jnp.clip(jnp.exp(math.log(0.004) - 3.6888795 * jax.random.uniform(streams_of[5], (LAYERS, D, KV), jnp.float32) ** block_levels(streams_of[5], (LAYERS, D, KV), ((1, 8), (2, 4)), -0.2, 0.2)), 0.0001, 0.004),
    }


def reference(partials, token_counts, owner_map, params, moment1, moment2):
    weights = token_counts.astype(jnp.float32)
    total = jnp.sum(weights)

    def accumulate(summed, pair):
        term, weight = pair
        return (summed + weight * term.astype(jnp.float32), None)
    summed, _ = lax.scan(accumulate, jnp.zeros((LAYERS, D, KV), jnp.float32), (partials, weights))
    grad = summed / total
    first = 0.9 * moment1 + 0.1 * grad
    second = 0.999 * moment2 + 0.001 * grad * grad
    bias_one = 1.0 - 0.9 ** STEP
    bias_two = 1.0 - 0.999 ** STEP
    direction = first / bias_one / (jnp.sqrt(second / bias_two) + 1e-08)
    new_params = params - 0.001 * (direction + 0.1 * params)
    delta = direction.astype(jnp.bfloat16)
    blocks = delta.reshape(LAYERS, D, N_TP, KV // N_TP)
    chosen = owner_map.astype(jnp.int32)[:, None, :, None]
    rollout = jnp.take_along_axis(blocks, chosen, axis=2).reshape(LAYERS, D, KV)
    return (new_params, first, second, rollout)
```

```python
import functools

import jax
import jax.numpy as jnp
from jax import lax
from jax.experimental import pallas as pl
from jax.experimental.pallas import tpu as pltpu
from jax.sharding import PartitionSpec as P

STEP = 10
MESH = pl.DeviceIdType.MESH
SPLIT = 4
TILE = 16


def plain(partials, token_counts, owner_map, params, moment1, moment2):
    weight = token_counts.astype(jnp.float32)[0]
    total = lax.psum(weight, "fsdp")
    summed = lax.psum_scatter(
        weight * partials[0].astype(jnp.float32), "fsdp", scatter_dimension=1, tiled=True
    )
    first, second, direction, new_params = adam(summed * (1.0 / total), params, moment1, moment2)
    delta = direction.astype(jnp.bfloat16)
    owners = lax.axis_size("tp")
    served = lax.dynamic_index_in_dim(owner_map, lax.axis_index("tp"), 1, keepdims=False)
    blocks = lax.all_gather(delta, "tp", axis=0)
    kept = jnp.take_along_axis(blocks, served[None, :, None, None], axis=0)[0]
    rollout = lax.all_gather(kept, "fsdp", axis=1, tiled=True)
    return (new_params, first, second, rollout)


def adam(grad, params, moment1, moment2):
    first = 0.9 * moment1 + 0.1 * grad
    second = 0.999 * moment2 + 0.001 * grad * grad
    scale_one = 1.0 / (1.0 - 0.9**STEP)
    scale_two = 1.0 / (1.0 - 0.999**STEP)
    direction = first * scale_one / (jnp.sqrt(second * scale_two) + 1e-08)
    new_params = params - 0.001 * (direction + 0.1 * params)
    return first, second, direction, new_params


def kernel(
    sizes,
    owner_ref,
    w_ref,
    part_ref,
    p_ref,
    m_ref,
    v_ref,
    np_ref,
    nm_ref,
    nv_ref,
    roll_ref,
    wbuf,
    mine,
    theirs,
    acc,
    recv,
    pbuf,
    mbuf,
    vbuf,
    dsend,
    zrecv,
    ag,
    w_s,
    w_r,
    opt_s,
    ld_s,
    raw_s,
    raw_r,
    rs_s,
    rs_r,
    z_s,
    z_r,
    ag_s,
    ag_r,
    fin_s,
    fin_r,
    out_s,
    upd_s,
):
    layers, fsdp, tp, parts, rows = sizes
    chunks = layers * parts
    pairs = fsdp // 2
    bits = pairs.bit_length() - 1
    me = lax.axis_index("fsdp")
    col = lax.axis_index("tp")
    core = lax.rem(me, 2)
    mine_q = me // 2
    partner = mine_q * 2 + (1 - core)

    barrier = pltpu.get_barrier_semaphore()
    for d in range(1, fsdp):
        pl.semaphore_signal(
            barrier, inc=1, device_id={"fsdp": lax.rem(me + d, fsdp)}, device_id_type=MESH
        )
    for d in range(1, tp):
        pl.semaphore_signal(
            barrier, inc=1, device_id={"tp": lax.rem(col + d, tp)}, device_id_type=MESH
        )

    def where(c):
        return c // parts, c % parts

    ends = []
    loads = []
    for c in range(chunks):
        l, k = where(c)
        load = pltpu.make_async_copy(part_ref.at[l, :, core, k], mine.at[c], ld_s.at[c])
        load.start()
        loads.append(load)
    opts = []
    for i, (src, dst) in enumerate(((p_ref, pbuf), (m_ref, mbuf), (v_ref, vbuf))):
        load = pltpu.make_async_copy(src, dst, opt_s.at[i])
        load.start()
        opts.append(load)

    pl.semaphore_wait(barrier, fsdp - 1 + tp - 1)

    def push(src, dst, send, arrive, **device):
        copy = pltpu.make_async_remote_copy(
            src_ref=src,
            dst_ref=dst,
            send_sem=send,
            recv_sem=arrive,
            device_id=device,
            device_id_type=MESH,
        )
        copy.start()
        return copy

    weights = []
    for d in range(1, fsdp):
        weights.append(
            push(w_ref, wbuf.at[d], w_s.at[d], w_r.at[d], fsdp=lax.rem(me + d, fsdp))
        )
    raws = []
    for c in range(chunks):
        l, k = where(c)
        raws.append(
            push(
                part_ref.at[l, :, 1 - core, k],
                theirs.at[c],
                raw_s.at[c],
                raw_r.at[c],
                fsdp=partner,
            )
        )
    for copy in weights:
        copy.wait()
    my_weight = w_ref[0:1, :]
    total = my_weight
    for d in range(1, fsdp):
        total = total + wbuf[d, 0:1, :]
    other_weight = jnp.where(core == 1, wbuf[1, 0:1, :], wbuf[fsdp - 1, 0:1, :])
    scale = 1.0 / total

    def order(c):
        names = list(range(bits))
        return names if c % 2 == 0 else names[::-1]

    def flipped(flips):
        q = mine_q
        for b in flips:
            q = q + (1 - 2 * lax.rem(mine_q // (1 << b), 2)) * (1 << b)
        return q

    step = 2 * TILE if rows % (2 * TILE) == 0 else TILE

    def tiles(body):
        def run(i, carry):
            body(pl.ds(pl.multiple_of(i * step, step), step))
            return carry

        lax.fori_loop(0, rows // step, run, 0)

    halving = {}
    spread = {}
    doubling = {}

    def halve(c, i):
        half = pairs >> (i + 1)
        there = flipped([order(c)[i]]) * 2 + core
        halving[c, i] = push(
            acc.at[c, pl.ds(half, half)],
            recv.at[c, pl.ds(half, half)],
            rs_s.at[c, i],
            rs_r.at[c, i],
            fsdp=there,
        )

    def double(c, j):
        size = 1 << j
        there = flipped([order(c)[j]]) * 2 + core
        doubling[c, j] = push(
            ag.at[c, pl.ds(0, size)],
            ag.at[c, pl.ds(size, size)],
            ag_s.at[c, j],
            ag_r.at[c, j],
            fsdp=there,
        )

    def gather_sum(c):
        loads[c].wait()
        raws[c].wait_recv()
        for pos in range(pairs - 1, -1, -1):
            q = flipped([order(c)[i] for i in range(bits) if pos >> (bits - 1 - i) & 1])

            def body(at):
                acc[c, pos, at, :] = my_weight * mine[c, q, at, :].astype(
                    jnp.float32
                ) + other_weight * theirs[c, q, at, :].astype(jnp.float32)

            tiles(body)
            if pos == pairs // 2:
                halve(c, 0)

    def add(i, c):
        halving[c, i].wait_recv()
        half = pairs >> (i + 1)
        for pos in range(half - 1, -1, -1):

            def body(at):
                acc[c, pos, at, :] = acc[c, pos, at, :] + recv[c, half + pos, at, :]

            tiles(body)
            if pos == half // 2:
                halve(c, i + 1)

    def update(c):
        l, k = where(c)
        halving[c, bits - 1].wait_recv()
        if c == 0:
            for load in opts:
                load.wait()

        def body(at):
            grad = (acc[c, 0, at, :] + recv[c, 1, at, :]) * scale
            first, second, direction, new_params = adam(
                grad, pbuf[l, k, at, :], mbuf[l, k, at, :], vbuf[l, k, at, :]
            )
            dsend[c, at, :] = direction.astype(jnp.bfloat16)
            pbuf[l, k, at, :] = new_params
            mbuf[l, k, at, :] = first
            vbuf[l, k, at, :] = second

        tiles(body)
        for d in range(1, tp):
            spread[c, d] = push(
                dsend.at[c],
                zrecv.at[c, d - 1],
                z_s.at[c, d - 1],
                z_r.at[c, d - 1],
                tp=lax.rem(col + d, tp),
            )
        for i, (src, dst) in enumerate(((pbuf, np_ref), (mbuf, nm_ref), (vbuf, nv_ref))):
            copy = pltpu.make_async_copy(src.at[l, k], dst.at[l, k], upd_s.at[c, i])
            copy.start()
            ends.append(copy.wait)

    def select(c):
        l, k = where(c)
        for d in range(1, tp):
            spread[c, d].wait_recv()
        served = owner_ref[l, col]

        def body(at):
            kept = dsend[c, at, :].astype(jnp.float32)
            for d in range(1, tp):
                kept = jnp.where(
                    served == lax.rem(col + (tp - d), tp),
                    zrecv[c, d - 1, at, :].astype(jnp.float32),
                    kept,
                )
            ag[c, 0, at, :] = kept.astype(jnp.bfloat16)

        tiles(body)
        double(c, 0)

    def finish(c, first, count):
        l, k = where(c)
        for pos in range(first, first + count):
            q = flipped([order(c)[j] for j in range(bits) if pos >> j & 1])
            local = pltpu.make_async_copy(ag.at[c, pos], roll_ref.at[l, q, core, k], out_s.at[c])
            local.start()
            push(
                ag.at[c, pos], roll_ref.at[l, q, core, k], fin_s.at[c], fin_r.at[c], fsdp=partner
            )

    def forward(j, c):
        doubling[c, j].wait_recv()
        if j + 1 < bits:
            double(c, j + 1)
        if j == 0:
            finish(c, 0, 1)
        finish(c, 1 << j, 1 << j)

    stages = [gather_sum]
    stages += [functools.partial(add, i) for i in range(bits - 1)]
    stages += [update, select]
    stages += [functools.partial(forward, j) for j in range(bits)]
    groups = [tuple(range(c, min(c + 2, chunks))) for c in range(0, chunks, 2)]
    for t in range(len(groups) + len(stages) - 1):
        for s, stage in enumerate(stages):
            if 0 <= t - s < len(groups):
                for c in groups[t - s]:
                    stage(c)

    for c in range(chunks):
        raws[c].wait_send()
        for i in range(bits):
            halving[c, i].wait_send()
            doubling[c, i].wait_send()
        for d in range(1, tp):
            spread[c, d].wait_send()
        for sem in (out_s, fin_s, fin_r):
            pltpu.make_async_copy(ag.at[c], ag.at[c], sem.at[c]).wait()
    for wait in ends:
        wait()


def fused(fsdp, tp, partials, token_counts, owner_map, params, moment1, moment2):
    layers, depth, width = partials.shape[1:]
    per = params.shape[1]
    pairs = fsdp // 2
    bits = pairs.bit_length() - 1
    parts = next(n for n in range(SPLIT, 0, -1) if per % (n * TILE) == 0)
    rows = per // parts
    chunks = layers * parts
    weight = jnp.broadcast_to(token_counts.astype(jnp.float32)[:, None], (8, width))
    anywhere = pl.BlockSpec(memory_space=pl.ANY)
    dma = pltpu.SemaphoreType.DMA
    state = (layers, parts, rows, width)
    f32, b16 = jnp.float32, jnp.bfloat16
    outs = pl.pallas_call(
        functools.partial(kernel, (layers, fsdp, tp, parts, rows)),
        out_shape=[
            jax.ShapeDtypeStruct(state, f32),
            jax.ShapeDtypeStruct(state, f32),
            jax.ShapeDtypeStruct(state, f32),
            jax.ShapeDtypeStruct((layers, pairs, 2, parts, rows, width), b16),
        ],
        in_specs=[
            pl.BlockSpec(memory_space=pltpu.SMEM),
            pl.BlockSpec(memory_space=pltpu.VMEM),
            anywhere,
            anywhere,
            anywhere,
            anywhere,
        ],
        out_specs=[anywhere] * 4,
        scratch_shapes=[
            pltpu.VMEM((fsdp, 8, width), f32),
            pltpu.VMEM((chunks, pairs, rows, width), b16),
            pltpu.VMEM((chunks, pairs, rows, width), b16),
            pltpu.VMEM((chunks, pairs, rows, width), f32),
            pltpu.VMEM((chunks, pairs, rows, width), f32),
            pltpu.VMEM(state, f32),
            pltpu.VMEM(state, f32),
            pltpu.VMEM(state, f32),
            pltpu.VMEM((chunks, rows, width), b16),
            pltpu.VMEM((chunks, tp - 1, rows, width), b16),
            pltpu.VMEM((chunks, pairs, rows, width), b16),
            dma((fsdp,)),
            dma((fsdp,)),
            dma((3,)),
            dma((chunks,)),
            dma((chunks,)),
            dma((chunks,)),
            dma((chunks, bits)),
            dma((chunks, bits)),
            dma((chunks, tp - 1)),
            dma((chunks, tp - 1)),
            dma((chunks, bits)),
            dma((chunks, bits)),
            dma((chunks,)),
            dma((chunks,)),
            dma((chunks,)),
            dma((chunks, 3)),
        ],
        compiler_params=pltpu.CompilerParams(
            collective_id=0, has_side_effects=True, vmem_limit_bytes=56 * 1024 * 1024
        ),
    )(
        owner_map,
        weight,
        partials.reshape(layers, pairs, 2, parts, rows, width),
        params.reshape(state),
        moment1.reshape(state),
        moment2.reshape(state),
    )
    return (*(out.reshape(params.shape) for out in outs[:3]), outs[3].reshape(layers, depth, width))


def solution(mesh):
    fsdp, tp = mesh.shape["fsdp"], mesh.shape["tp"]
    local = plain
    if fsdp >= 4 and fsdp & (fsdp - 1) == 0 and tp > 1:
        local = functools.partial(fused, fsdp, tp)
    in_specs = (
        P("fsdp", None, None, "tp"),
        P("fsdp"),
        P(),
        P(None, "fsdp", "tp"),
        P(None, "fsdp", "tp"),
        P(None, "fsdp", "tp"),
    )
    out_specs = (
        P(None, "fsdp", "tp"),
        P(None, "fsdp", "tp"),
        P(None, "fsdp", "tp"),
        P(None, None, "tp"),
    )
    return jax.shard_map(local, mesh=mesh, in_specs=in_specs, out_specs=out_specs, check_vma=False)
```

```python
import functools

import jax
import jax.numpy as jnp
from jax import lax
from jax.experimental import pallas as pl
from jax.experimental.pallas import tpu as pltpu
from jax.sharding import PartitionSpec as P

STEP = 10
MESH = pl.DeviceIdType.MESH
SPLIT = 4
TILE = 16


def plain(partials, token_counts, owner_map, params, moment1, moment2):
    weight = token_counts.astype(jnp.float32)[0]
    total = lax.psum(weight, "fsdp")
    summed = lax.psum_scatter(
        weight * partials[0].astype(jnp.float32), "fsdp", scatter_dimension=1, tiled=True
    )
    first, second, direction, new_params = adam(summed * (1.0 / total), params, moment1, moment2)
    delta = direction.astype(jnp.bfloat16)
    owners = lax.axis_size("tp")
    served = lax.dynamic_index_in_dim(owner_map, lax.axis_index("tp"), 1, keepdims=False)
    blocks = lax.all_gather(delta, "tp", axis=0)
    kept = jnp.take_along_axis(blocks, served[None, :, None, None], axis=0)[0]
    rollout = lax.all_gather(kept, "fsdp", axis=1, tiled=True)
    return (new_params, first, second, rollout)


def adam(grad, params, moment1, moment2):
    first = 0.9 * moment1 + 0.1 * grad
    second = 0.999 * moment2 + 0.001 * grad * grad
    scale_one = 1.0 / (1.0 - 0.9**STEP)
    scale_two = 1.0 / (1.0 - 0.999**STEP)
    direction = first * scale_one / (jnp.sqrt(second * scale_two) + 1e-08)
    new_params = params - 0.001 * (direction + 0.1 * params)
    return first, second, direction, new_params


def kernel(
    sizes,
    owner_ref,
    w_ref,
    part_ref,
    p_ref,
    m_ref,
    v_ref,
    np_ref,
    nm_ref,
    nv_ref,
    roll_ref,
    wbuf,
    mine,
    theirs,
    acc,
    recv,
    held,
    cross,
    w_s,
    w_r,
    opt_s,
    ld_s,
    raw_s,
    raw_r,
    rs_s,
    rs_r,
    z_s,
    z_r,
    ag_s,
    ag_r,
    fin_s,
    fin_r,
):
    layers, fsdp, tp, parts, rows = sizes
    chunks = layers * parts
    pairs = fsdp // 2
    bits = pairs.bit_length() - 1
    me = lax.axis_index("fsdp")
    col = lax.axis_index("tp")
    core = lax.rem(me, 2)
    mine_q = me // 2
    partner = mine_q * 2 + (1 - core)

    def away(index, flips):
        q = index
        for b in flips:
            q = q + (1 - 2 * lax.rem(index // (1 << b), 2)) * (1 << b)
        return q

    def ones(number):
        return [b for b in range(number.bit_length()) if number >> b & 1]

    tp_bits = tp.bit_length() - 1
    barrier = pltpu.get_barrier_semaphore()
    for d in range(1, fsdp):
        pl.semaphore_signal(
            barrier, inc=1, device_id={"fsdp": lax.rem(me + d, fsdp)}, device_id_type=MESH
        )
    for b in range(tp_bits):
        pl.semaphore_signal(
            barrier, inc=1, device_id={"tp": away(col, [b])}, device_id_type=MESH
        )

    def where(c):
        return c // parts, c % parts

    loads = []
    for c in range(chunks):
        l, k = where(c)
        load = pltpu.make_async_copy(part_ref.at[l, :, core, k], mine.at[c], ld_s.at[c])
        load.start()
        loads.append(load)
    opts = []
    for i, (src, dst) in enumerate(((p_ref, np_ref), (m_ref, nm_ref), (v_ref, nv_ref))):
        load = pltpu.make_async_copy(src, dst, opt_s.at[i])
        load.start()
        opts.append(load)

    pl.semaphore_wait(barrier, fsdp - 1 + tp_bits)

    def push(src, dst, send, arrive, **device):
        copy = pltpu.make_async_remote_copy(
            src_ref=src,
            dst_ref=dst,
            send_sem=send,
            recv_sem=arrive,
            device_id=device,
            device_id_type=MESH,
        )
        copy.start()
        return copy

    weights = []
    for d in range(1, fsdp):
        weights.append(
            push(w_ref, wbuf.at[d], w_s.at[d], w_r.at[d], fsdp=lax.rem(me + d, fsdp))
        )
    raws = []
    for c in range(chunks):
        l, k = where(c)
        raws.append(
            push(
                part_ref.at[l, :, 1 - core, k],
                theirs.at[c],
                raw_s.at[c],
                raw_r.at[c],
                fsdp=partner,
            )
        )
    for copy in weights:
        copy.wait()
    my_weight = w_ref[0:1, :]
    total = my_weight
    for d in range(1, fsdp):
        total = total + wbuf[d, 0:1, :]
    other_weight = jnp.where(core == 1, wbuf[1, 0:1, :], wbuf[fsdp - 1, 0:1, :])
    scale = 1.0 / total

    def order(c):
        names = list(range(bits))
        return names if c % 2 == 0 else names[::-1]

    def flipped(flips):
        return away(mine_q, flips)

    step = 2 * TILE if rows % (2 * TILE) == 0 else TILE

    def tiles(body):
        def run(i, carry):
            body(pl.ds(pl.multiple_of(i * step, step), step))
            return carry

        lax.fori_loop(0, rows // step, run, 0)

    halving = {}
    spread = {}
    doubling = {}

    def halve(c, i):
        half = pairs >> (i + 1)
        there = flipped([order(c)[i]]) * 2 + core
        halving[c, i] = push(
            acc.at[c, pl.ds(half, half)],
            recv.at[c, pl.ds(half, half)],
            rs_s.at[c, i],
            rs_r.at[c, i],
            fsdp=there,
        )

    def held_rows(c, pos):
        q = flipped([order(c)[b] for b in ones(pos)])
        l, k = where(c)
        return roll_ref.at[l, q, core, k]

    def double(c, j):
        there = flipped([order(c)[j]]) * 2 + core
        for pos in range(1 << j):
            block = held_rows(c, pos)
            push(block, block, ag_s.at[c, j], ag_r.at[c, j], fsdp=there)

    def await_blocks(c, count, sem):
        part = mine.at[c, pl.ds(0, count)]
        pltpu.make_async_copy(part, part, sem).wait()

    def gather_sum(c):
        loads[c].wait()
        raws[c].wait_recv()
        for pos in range(pairs - 1, -1, -1):
            q = flipped([order(c)[i] for i in range(bits) if pos >> (bits - 1 - i) & 1])

            def body(at):
                acc[c, pos, at, :] = my_weight * mine[c, q, at, :].astype(
                    jnp.float32
                ) + other_weight * theirs[c, q, at, :].astype(jnp.float32)

            tiles(body)
            if pos == pairs // 2:
                halve(c, 0)

    def add(i, c):
        halving[c, i].wait_recv()
        half = pairs >> (i + 1)
        for pos in range(half - 1, -1, -1):

            def body(at):
                acc[c, pos, at, :] = acc[c, pos, at, :] + recv[c, half + pos, at, :]

            tiles(body)
            if pos == half // 2:
                halve(c, i + 1)

    def update(c):
        l, k = where(c)
        halving[c, bits - 1].wait_recv()
        if c == 0:
            for load in opts:
                load.wait()

        def body(at):
            grad = (acc[c, 0, at, :] + recv[c, 1, at, :]) * scale
            first, second, direction, new_params = adam(
                grad, np_ref[l, k, at, :], nm_ref[l, k, at, :], nv_ref[l, k, at, :]
            )
            held[c, 0, at, :] = direction.astype(jnp.bfloat16)
            np_ref[l, k, at, :] = new_params
            nm_ref[l, k, at, :] = first
            nv_ref[l, k, at, :] = second

        tiles(body)
        if tp_bits > 1:
            meet(c, 0)
        else:
            hand_over(c)

    def meet(c, b):
        size = 1 << b
        spread[c, b] = push(
            held.at[c, pl.ds(0, size)],
            held.at[c, pl.ds(size, size)],
            z_s.at[c, b],
            z_r.at[c, b],
            tp=away(col, [b]),
        )

    def pick(c, at, served, start):
        kept = start
        for slot in range(tp // 2):
            kept = jnp.where(
                served == away(col, ones(slot)), held[c, slot, at, :].astype(jnp.float32), kept
            )
        return kept.astype(jnp.bfloat16)

    def hand_over(c):
        l, k = where(c)
        there = away(col, [tp_bits - 1])
        served = owner_ref[l, there]

        def body(at):
            cross[c, 0, at, :] = pick(c, at, served, held[c, 0, at, :].astype(jnp.float32))

        tiles(body)
        spread[c, tp_bits - 1] = push(
            cross.at[c, 0],
            cross.at[c, 1],
            z_s.at[c, tp_bits - 1],
            z_r.at[c, tp_bits - 1],
            tp=there,
        )

    def met(b, c):
        spread[c, b].wait_recv()
        if b + 2 < tp_bits:
            meet(c, b + 1)
        else:
            hand_over(c)

    def select(c):
        l, k = where(c)
        spread[c, tp_bits - 1].wait_recv()
        served = owner_ref[l, col]

        def body(at):
            roll_ref[l, mine_q, core, k, at, :] = pick(
                c, at, served, cross[c, 1, at, :].astype(jnp.float32)
            )

        tiles(body)
        double(c, 0)
        finish(c, 0, 1)

    def finish(c, first, count):
        for pos in range(first, first + count):
            block = held_rows(c, pos)
            push(block, block, fin_s.at[c], fin_r.at[c], fsdp=partner)

    def forward(j, c):
        await_blocks(c, 1 << j, ag_r.at[c, j])
        if j + 1 < bits:
            double(c, j + 1)
        finish(c, 1 << j, 1 << j)

    stages = [gather_sum]
    stages += [functools.partial(add, i) for i in range(bits - 1)]
    stages += [update]
    stages += [functools.partial(met, b) for b in range(tp_bits - 1)]
    stages += [select]
    stages += [functools.partial(forward, j) for j in range(bits)]
    groups = [tuple(range(c, min(c + 2, chunks))) for c in range(0, chunks, 2)]
    for t in range(len(groups) + len(stages) - 1):
        for s, stage in enumerate(stages):
            if 0 <= t - s < len(groups):
                for c in groups[t - s]:
                    stage(c)

    for c in range(chunks):
        raws[c].wait_send()
        for i in range(bits):
            halving[c, i].wait_send()
            await_blocks(c, 1 << i, ag_s.at[c, i])
        for b in range(tp_bits):
            spread[c, b].wait_send()
        for sem in (fin_s, fin_r):
            await_blocks(c, pairs, sem.at[c])


def write_out(*refs):
    count = len(refs) // 2
    copies = []
    for i in range(count):
        for l in range(refs[i].shape[0]):
            sem = refs[-1].at[i, l]
            copies.append(pltpu.make_async_copy(refs[i].at[l], refs[count + i].at[l], sem))
    for copy in copies:
        copy.start()
    for copy in copies:
        copy.wait()


def fused(fsdp, tp, partials, token_counts, owner_map, params, moment1, moment2):
    layers, depth, width = partials.shape[1:]
    per = params.shape[1]
    pairs = fsdp // 2
    bits = pairs.bit_length() - 1
    tp_bits = tp.bit_length() - 1
    parts = next(n for n in range(SPLIT, 0, -1) if per % (n * TILE) == 0)
    rows = per // parts
    chunks = layers * parts
    weight = jnp.broadcast_to(token_counts.astype(jnp.float32)[:, None], (8, width))
    anywhere = pl.BlockSpec(memory_space=pl.ANY)
    dma = pltpu.SemaphoreType.DMA
    state = (layers, parts, rows, width)
    f32, b16 = jnp.float32, jnp.bfloat16
    outs = pl.pallas_call(
        functools.partial(kernel, (layers, fsdp, tp, parts, rows)),
        out_shape=[
            pltpu.VMEM(state, f32),
            pltpu.VMEM(state, f32),
            pltpu.VMEM(state, f32),
            pltpu.VMEM((layers, pairs, 2, parts, rows, width), b16),
        ],
        in_specs=[
            pl.BlockSpec(memory_space=pltpu.SMEM),
            pl.BlockSpec(memory_space=pltpu.VMEM),
            anywhere,
            anywhere,
            anywhere,
            anywhere,
        ],
        out_specs=[pl.BlockSpec(memory_space=pltpu.VMEM)] * 4,
        scratch_shapes=[
            pltpu.VMEM((fsdp, 8, width), f32),
            pltpu.VMEM((chunks, pairs, rows, width), b16),
            pltpu.VMEM((chunks, pairs, rows, width), b16),
            pltpu.VMEM((chunks, pairs, rows, width), f32),
            pltpu.VMEM((chunks, pairs, rows, width), f32),
            pltpu.VMEM((chunks, tp // 2, rows, width), b16),
            pltpu.VMEM((chunks, 2, rows, width), b16),
            dma((fsdp,)),
            dma((fsdp,)),
            dma((3,)),
            dma((chunks,)),
            dma((chunks,)),
            dma((chunks,)),
            dma((chunks, bits)),
            dma((chunks, bits)),
            dma((chunks, tp_bits)),
            dma((chunks, tp_bits)),
            dma((chunks, bits)),
            dma((chunks, bits)),
            dma((chunks,)),
            dma((chunks,)),
        ],
        compiler_params=pltpu.CompilerParams(
            collective_id=0, has_side_effects=True, vmem_limit_bytes=48 * 1024 * 1024
        ),
    )(
        owner_map,
        weight,
        partials.reshape(layers, pairs, 2, parts, rows, width),
        params.reshape(state),
        moment1.reshape(state),
        moment2.reshape(state),
    )
    outs = [out.reshape(params.shape) for out in outs[:3]] + [outs[3].reshape(layers, depth, width)]
    return tuple(
        pl.pallas_call(
            write_out,
            out_shape=[jax.ShapeDtypeStruct(out.shape, out.dtype) for out in outs],
            in_specs=[pl.BlockSpec(memory_space=pltpu.VMEM)] * 4,
            out_specs=[anywhere] * 4,
            scratch_shapes=[dma((4, layers))],
            compiler_params=pltpu.CompilerParams(vmem_limit_bytes=16 * 1024 * 1024),
        )(*outs)
    )


def solution(mesh):
    fsdp, tp = mesh.shape["fsdp"], mesh.shape["tp"]
    local = plain
    if fsdp >= 4 and fsdp & (fsdp - 1) == 0 and tp > 1 and tp & (tp - 1) == 0:
        local = functools.partial(fused, fsdp, tp)
    in_specs = (
        P("fsdp", None, None, "tp"),
        P("fsdp"),
        P(),
        P(None, "fsdp", "tp"),
        P(None, "fsdp", "tp"),
        P(None, "fsdp", "tp"),
    )
    out_specs = (
        P(None, "fsdp", "tp"),
        P(None, "fsdp", "tp"),
        P(None, "fsdp", "tp"),
        P(None, None, "tp"),
    )
    return jax.shard_map(local, mesh=mesh, in_specs=in_specs, out_specs=out_specs, check_vma=False)
```

```python
import functools

import jax
import jax.numpy as jnp
from jax import lax
from jax.experimental import pallas as pl
from jax.experimental.pallas import tpu as pltpu
from jax.sharding import PartitionSpec as P

STEP = 10
MESH = pl.DeviceIdType.MESH
SPLIT = 8
TILE = 16
SPAN = 80


def plain(partials, token_counts, owner_map, params, moment1, moment2):
    weight = token_counts.astype(jnp.float32)[0]
    total = lax.psum(weight, "fsdp")
    summed = lax.psum_scatter(
        weight * partials[0].astype(jnp.float32), "fsdp", scatter_dimension=1, tiled=True
    )
    first, second, direction, new_params = adam(summed * (1.0 / total), params, moment1, moment2)
    delta = direction.astype(jnp.bfloat16)
    owners = lax.axis_size("tp")
    served = lax.dynamic_index_in_dim(owner_map, lax.axis_index("tp"), 1, keepdims=False)
    blocks = lax.all_gather(delta, "tp", axis=0)
    kept = jnp.take_along_axis(blocks, served[None, :, None, None], axis=0)[0]
    rollout = lax.all_gather(kept, "fsdp", axis=1, tiled=True)
    return (new_params, first, second, rollout)


def adam(grad, params, moment1, moment2):
    first = 0.9 * moment1 + 0.1 * grad
    second = 0.999 * moment2 + 0.001 * grad * grad
    scale_one = 1.0 / (1.0 - 0.9**STEP)
    scale_two = 1.0 / (1.0 - 0.999**STEP)
    direction = first * scale_one / (jnp.sqrt(second * scale_two) + 1e-08)
    new_params = params - 0.001 * (direction + 0.1 * params)
    return first, second, direction, new_params


def kernel(
    sizes,
    owner_ref,
    w_ref,
    part_ref,
    p_ref,
    m_ref,
    v_ref,
    np_ref,
    nm_ref,
    nv_ref,
    roll_ref,
    wbuf,
    mine,
    theirs,
    acc,
    recv,
    held,
    cross,
    w_s,
    w_r,
    opt_s,
    ld_s,
    raw_s,
    raw_r,
    rs_s,
    rs_r,
    z_s,
    z_r,
    ag_s,
    ag_r,
    fin_s,
    fin_r,
):
    layers, fsdp, tp, parts, rows = sizes
    chunks = layers * parts
    pairs = fsdp // 2
    bits = pairs.bit_length() - 1
    me = lax.axis_index("fsdp")
    col = lax.axis_index("tp")
    core = lax.rem(me, 2)
    mine_q = me // 2
    partner = mine_q * 2 + (1 - core)

    def away(index, flips):
        q = index
        for b in flips:
            q = q + (1 - 2 * lax.rem(index // (1 << b), 2)) * (1 << b)
        return q

    def ones(number):
        return [b for b in range(number.bit_length()) if number >> b & 1]

    tp_bits = tp.bit_length() - 1
    barrier = pltpu.get_barrier_semaphore()
    for d in range(1, fsdp):
        pl.semaphore_signal(
            barrier, inc=1, device_id={"fsdp": lax.rem(me + d, fsdp)}, device_id_type=MESH
        )
    for b in range(tp_bits):
        pl.semaphore_signal(
            barrier, inc=1, device_id={"tp": away(col, [b])}, device_id_type=MESH
        )

    def where(c):
        return c // parts, c % parts

    loads = []
    for c in range(chunks):
        l, k = where(c)
        load = pltpu.make_async_copy(part_ref.at[l, :, core, k], mine.at[c], ld_s.at[c])
        load.start()
        loads.append(load)
    pl.semaphore_wait(barrier, fsdp - 1 + tp_bits)

    def push(src, dst, send, arrive, **device):
        copy = pltpu.make_async_remote_copy(
            src_ref=src,
            dst_ref=dst,
            send_sem=send,
            recv_sem=arrive,
            device_id=device,
            device_id_type=MESH,
        )
        copy.start()
        return copy

    weights = [push(w_ref, wbuf.at[0], w_s.at[0], w_r.at[0], fsdp=partner)]
    raws = []
    for c in range(chunks):
        l, k = where(c)
        raws.append(
            push(
                part_ref.at[l, :, 1 - core, k],
                theirs.at[c],
                raw_s.at[c],
                raw_r.at[c],
                fsdp=partner,
            )
        )
    for d in range(1, fsdp):
        weights.append(
            push(w_ref, wbuf.at[d], w_s.at[d], w_r.at[d], fsdp=lax.rem(me + d, fsdp))
        )
    opts = []
    for i, (src, dst) in enumerate(((p_ref, np_ref), (m_ref, nm_ref), (v_ref, nv_ref))):
        load = pltpu.make_async_copy(src, dst, opt_s.at[i])
        load.start()
        opts.append(load)

    my_weight = w_ref[0:1, :]
    weights[0].wait()
    other_weight = wbuf[0, 0:1, :]

    def weigh():
        total = my_weight
        for d in range(1, fsdp):
            weights[d].wait()
            total = total + wbuf[d, 0:1, :]
        return 1.0 / total

    scale = []

    def order(c):
        names = list(range(bits))
        return names if c % 2 == 0 else names[::-1]

    def flipped(flips):
        return away(mine_q, flips)

    step = next(n for n in range(min(rows, SPAN), 0, -TILE) if rows % n == 0)

    def tiles(body):
        def run(i, carry):
            body(pl.ds(pl.multiple_of(i * step, step), step))
            return carry

        lax.fori_loop(0, rows // step, run, 0)

    halving = {}
    spread = {}
    doubling = {}

    def halve(c, i):
        half = pairs >> (i + 1)
        there = flipped([order(c)[i]]) * 2 + core
        halving[c, i] = push(
            acc.at[c, pl.ds(half, half)],
            recv.at[c, pl.ds(half, half)],
            rs_s.at[c, i],
            rs_r.at[c, i],
            fsdp=there,
        )

    def held_rows(c, pos):
        q = flipped([order(c)[b] for b in ones(pos)])
        l, k = where(c)
        return roll_ref.at[l, q, core, k]

    def double(c, j):
        there = flipped([order(c)[j]]) * 2 + core
        for pos in range(1 << j):
            block = held_rows(c, pos)
            push(block, block, ag_s.at[c, j], ag_r.at[c, j], fsdp=there)

    def await_blocks(c, count, sem):
        part = mine.at[c, pl.ds(0, count)]
        pltpu.make_async_copy(part, part, sem).wait()

    def gather_sum(c):
        loads[c].wait()
        raws[c].wait_recv()
        for pos in range(pairs - 1, -1, -1):
            q = flipped([order(c)[i] for i in range(bits) if pos >> (bits - 1 - i) & 1])

            def body(at):
                acc[c, pos, at, :] = my_weight * mine[c, q, at, :].astype(
                    jnp.float32
                ) + other_weight * theirs[c, q, at, :].astype(jnp.float32)

            tiles(body)
            if pos == pairs // 2:
                halve(c, 0)

    def add(i, c):
        halving[c, i].wait_recv()
        half = pairs >> (i + 1)
        for pos in range(half - 1, -1, -1):

            def body(at):
                acc[c, pos, at, :] = acc[c, pos, at, :] + recv[c, half + pos, at, :]

            tiles(body)
            if pos == half // 2:
                halve(c, i + 1)

    def update(c):
        l, k = where(c)
        halving[c, bits - 1].wait_recv()
        if c == 0:
            for load in opts:
                load.wait()
            scale.append(weigh())

        def body(at):
            grad = (acc[c, 0, at, :] + recv[c, 1, at, :]) * scale[0]
            first, second, direction, new_params = adam(
                grad, np_ref[l, k, at, :], nm_ref[l, k, at, :], nv_ref[l, k, at, :]
            )
            held[c, 0, at, :] = direction.astype(jnp.bfloat16)
            np_ref[l, k, at, :] = new_params
            nm_ref[l, k, at, :] = first
            nv_ref[l, k, at, :] = second

        tiles(body)
        if tp_bits > 1:
            meet(c, 0)
        else:
            hand_over(c)

    def meet(c, b):
        size = 1 << b
        spread[c, b] = push(
            held.at[c, pl.ds(0, size)],
            held.at[c, pl.ds(size, size)],
            z_s.at[c, b],
            z_r.at[c, b],
            tp=away(col, [b]),
        )

    def pick(c, at, served, start):
        kept = start
        for slot in range(tp // 2):
            kept = jnp.where(
                served == away(col, ones(slot)), held[c, slot, at, :].astype(jnp.float32), kept
            )
        return kept.astype(jnp.bfloat16)

    def hand_over(c):
        l, k = where(c)
        there = away(col, [tp_bits - 1])
        served = owner_ref[l, there]

        def body(at):
            cross[c, 0, at, :] = pick(c, at, served, held[c, 0, at, :].astype(jnp.float32))

        tiles(body)
        spread[c, tp_bits - 1] = push(
            cross.at[c, 0],
            cross.at[c, 1],
            z_s.at[c, tp_bits - 1],
            z_r.at[c, tp_bits - 1],
            tp=there,
        )

    def met(b, c):
        spread[c, b].wait_recv()
        if b + 2 < tp_bits:
            meet(c, b + 1)
        else:
            hand_over(c)

    def select(c):
        l, k = where(c)
        spread[c, tp_bits - 1].wait_recv()
        served = owner_ref[l, col]

        def body(at):
            roll_ref[l, mine_q, core, k, at, :] = pick(
                c, at, served, cross[c, 1, at, :].astype(jnp.float32)
            )

        tiles(body)
        double(c, 0)
        finish(c, 0, 1)

    def finish(c, first, count):
        for pos in range(first, first + count):
            block = held_rows(c, pos)
            push(block, block, fin_s.at[c], fin_r.at[c], fsdp=partner)

    def forward(j, c):
        await_blocks(c, 1 << j, ag_r.at[c, j])
        if j + 1 < bits:
            double(c, j + 1)
        finish(c, 1 << j, 1 << j)

    stages = [gather_sum]
    stages += [functools.partial(add, i) for i in range(bits - 1)]
    stages += [update]
    stages += [functools.partial(met, b) for b in range(tp_bits - 1)]
    stages += [select]
    stages += [functools.partial(forward, j) for j in range(bits)]
    groups = [tuple(range(c, min(c + 2, chunks))) for c in range(0, chunks, 2)]
    for t in range(len(groups) + len(stages) - 1):
        for s, stage in enumerate(stages):
            if 0 <= t - s < len(groups):
                for c in groups[t - s]:
                    stage(c)

    for c in range(chunks):
        raws[c].wait_send()
        for i in range(bits):
            halving[c, i].wait_send()
            await_blocks(c, 1 << i, ag_s.at[c, i])
        for b in range(tp_bits):
            spread[c, b].wait_send()
        for sem in (fin_s, fin_r):
            await_blocks(c, pairs, sem.at[c])


def write_out(*refs):
    count = len(refs) // 2
    copies = []
    for i in range(count):
        for l in range(refs[i].shape[0]):
            sem = refs[-1].at[i, l]
            copies.append(pltpu.make_async_copy(refs[i].at[l], refs[count + i].at[l], sem))
    for copy in copies:
        copy.start()
    for copy in copies:
        copy.wait()


def fused(fsdp, tp, partials, token_counts, owner_map, params, moment1, moment2):
    layers, depth, width = partials.shape[1:]
    per = params.shape[1]
    pairs = fsdp // 2
    bits = pairs.bit_length() - 1
    tp_bits = tp.bit_length() - 1
    parts = next(n for n in range(SPLIT, 0, -1) if per % (n * TILE) == 0)
    rows = per // parts
    chunks = layers * parts
    weight = jnp.broadcast_to(token_counts.astype(jnp.float32)[:, None], (8, width))
    anywhere = pl.BlockSpec(memory_space=pl.ANY)
    dma = pltpu.SemaphoreType.DMA
    state = (layers, parts, rows, width)
    f32, b16 = jnp.float32, jnp.bfloat16
    outs = pl.pallas_call(
        functools.partial(kernel, (layers, fsdp, tp, parts, rows)),
        out_shape=[
            pltpu.VMEM(state, f32),
            pltpu.VMEM(state, f32),
            pltpu.VMEM(state, f32),
            pltpu.VMEM((layers, pairs, 2, parts, rows, width), b16),
        ],
        in_specs=[
            pl.BlockSpec(memory_space=pltpu.SMEM),
            pl.BlockSpec(memory_space=pltpu.VMEM),
            anywhere,
            anywhere,
            anywhere,
            anywhere,
        ],
        out_specs=[pl.BlockSpec(memory_space=pltpu.VMEM)] * 4,
        scratch_shapes=[
            pltpu.VMEM((fsdp, 8, width), f32),
            pltpu.VMEM((chunks, pairs, rows, width), b16),
            pltpu.VMEM((chunks, pairs, rows, width), b16),
            pltpu.VMEM((chunks, pairs, rows, width), f32),
            pltpu.VMEM((chunks, pairs, rows, width), f32),
            pltpu.VMEM((chunks, tp // 2, rows, width), b16),
            pltpu.VMEM((chunks, 2, rows, width), b16),
            dma((fsdp,)),
            dma((fsdp,)),
            dma((3,)),
            dma((chunks,)),
            dma((chunks,)),
            dma((chunks,)),
            dma((chunks, bits)),
            dma((chunks, bits)),
            dma((chunks, tp_bits)),
            dma((chunks, tp_bits)),
            dma((chunks, bits)),
            dma((chunks, bits)),
            dma((chunks,)),
            dma((chunks,)),
        ],
        compiler_params=pltpu.CompilerParams(
            collective_id=0, has_side_effects=True, vmem_limit_bytes=48 * 1024 * 1024
        ),
    )(
        owner_map,
        weight,
        partials.reshape(layers, pairs, 2, parts, rows, width),
        params.reshape(state),
        moment1.reshape(state),
        moment2.reshape(state),
    )
    outs = [out.reshape(params.shape) for out in outs[:3]] + [outs[3].reshape(layers, depth, width)]
    return tuple(
        pl.pallas_call(
            write_out,
            out_shape=[jax.ShapeDtypeStruct(out.shape, out.dtype) for out in outs],
            in_specs=[pl.BlockSpec(memory_space=pltpu.VMEM)] * 4,
            out_specs=[anywhere] * 4,
            scratch_shapes=[dma((4, layers))],
            compiler_params=pltpu.CompilerParams(vmem_limit_bytes=16 * 1024 * 1024),
        )(*outs)
    )


def solution(mesh):
    fsdp, tp = mesh.shape["fsdp"], mesh.shape["tp"]
    local = plain
    if fsdp >= 4 and fsdp & (fsdp - 1) == 0 and tp > 1 and tp & (tp - 1) == 0:
        local = functools.partial(fused, fsdp, tp)
    in_specs = (
        P("fsdp", None, None, "tp"),
        P("fsdp"),
        P(),
        P(None, "fsdp", "tp"),
        P(None, "fsdp", "tp"),
        P(None, "fsdp", "tp"),
    )
    out_specs = (
        P(None, "fsdp", "tp"),
        P(None, "fsdp", "tp"),
        P(None, "fsdp", "tp"),
        P(None, None, "tp"),
    )
    return jax.shard_map(local, mesh=mesh, in_specs=in_specs, out_specs=out_specs, check_vma=False)
```
